256 devices in a mesh: ulysses: 16 (over z, x_hi), blk: 16 (over y, x_lo, core).
Axes of the slice: x: 4 (x_hi: 2, x_lo: 2; x = x_hi * 2 + x_lo), y: 4, z: 8, core: 2. Of those that a mesh axis runs over, the one named last changes fastest.
Arguments:
- queries: bfloat16 [16, 1024, 4096], P('blk', 'ulysses'), may hold values from -6 to 6
- key_rows: bfloat16 [16, 1024, 1024], P('blk', 'ulysses'), may hold values from -6 to 6
- value_rows: bfloat16 [16, 1024, 1024], P('blk', 'ulysses'), may hold values from -6 to 6
- tile_segment: int32 [128], replicated, may hold values from 0 to 31, never falling along the last dimension, each value on 1 to 8 neighbouring positions
Outputs:
- attended: bfloat16 [16, 1024, 4096], P('blk', 'ulysses')
The draws below stay inside these ranges and needn't reach their ends.
Inputs may be any that keep to these rules, and one draw needn't show every extreme that they name: `tile_segment`: segment numbers never fall along the sequence and each segment covers 1 to 8 tiles.
All inputs are finite; a program needn't handle non-finite values.
Results may differ from the reference program's by a relative error of at most 0.0045.
Values may be sent and summed in bfloat16 or wider, within the bound.
No kernel may reach another device: no remote copies, remote signals or barrier semaphores. Data moves between devices by JAX's collectives and lax.ppermute only.
A program may use at most 64 MiB of HBM per device.

```python
import math
import jax
import jax.numpy as jnp
import numpy as np
from jax import lax

Q_HEADS = 32
KV_HEADS = 8
HEAD_DIM = 128
TILE = 128
BLOCK_LEN = 1024
BLOCKS = 16
TILES = 128


def draw_queries(key, part):
    seq_total = BLOCKS * BLOCK_LEN
    row_width = Q_HEADS * HEAD_DIM
    noise_key = jax.random.fold_in(key, 101)
    sample = jnp.clip(1.6 * jax.random.normal(noise_key, (seq_total, row_width), jnp.float32), -6.0, 6.0)
    return sample.reshape(BLOCKS, BLOCK_LEN, row_width).astype(jnp.bfloat16)


def draw_key_rows(key, part):
    seq_total = BLOCKS * BLOCK_LEN
    row_width = KV_HEADS * HEAD_DIM
    noise_key = jax.random.fold_in(key, 202)
    sample = jnp.clip(1.6 * jax.random.normal(noise_key, (seq_total, row_width), jnp.float32), -6.0, 6.0)
    return sample.reshape(BLOCKS, BLOCK_LEN, row_width).astype(jnp.bfloat16)


def block_levels(stream_key, extent, pieces, low, high):
    loudness = 1.0
    for axis_at, shards_of in pieces:
        draws = jax.random.uniform(jax.random.fold_in(jax.random.fold_in(stream_key, 6), axis_at), (shards_of,), jnp.float32, low / len(pieces), high / len(pieces))
        loudness = loudness * jnp.repeat(jnp.exp(draws), extent[axis_at] // shards_of).reshape((-1,) + (1,) * (len(extent) - 1 - axis_at))
    return loudness


def profile(amount, total, bound, skew):
    loads = [(1 << 20) // math.isqrt(standing ** skew) + 1 for standing in range(2, amount + 1)]
    rest, given = total - bound - (amount - 1), [1] * (amount - 1)
    while rest > 0:
        free = [i for i in range(amount - 1) if given[i] < bound]
        mass, budget = sum([loads[i] for i in free]), rest
        for i in free:
            more = min(bound - given[i], max(1, budget * loads[i] // mass), rest)
            given[i] = given[i] + more
            rest = rest - more
    return np.array([bound] + given)


def ragged_sizes(key, amount, total, reach, slope):
    if amount == 2:
        one = jax.random.randint(key, (), max(1, total - reach), min(reach, total - 1) + 1)
        return jnp.stack([one, total - one])
    sizes = jnp.asarray(profile(amount, total, reach, slope), jnp.int32)
    couples = (amount - 1) // 2
    giver, sink = sizes[1:1 + 2 * couples:2], sizes[2:2 + 2 * couples:2]
    margin = jnp.minimum(giver - 1, reach - sink)
    passed = jax.random.randint(jax.random.fold_in(key, 1), (couples,), 0, 1 << 20) % (margin + 1)
    sizes = sizes.at[1:1 + 2 * couples:2].set(giver - passed).at[2:2 + 2 * couples:2].set(sink + passed)
    return sizes[jax.random.permutation(jax.random.fold_in(key, 2), amount)]


def bell_draw(stream_key, extent, deviation, bound, shards=(), held_as=jnp.bfloat16):
    values = jax.random.normal(stream_key, extent, jnp.float32) * deviation
    if len(shards) > 0:
        values = block_levels(stream_key, extent, shards, -0.22, 0.18) * values
    return jnp.clip(values, min=-bound, max=bound).astype(held_as)


def setup_inputs(seed: int = 0) -> dict:
    key_of = jax.random.split(jax.random.key(seed), 5)
    queries = draw_queries(jax.random.fold_in(key_of[4], 71), 0)
    key_rows = draw_key_rows(jax.random.fold_in(key_of[4], 71), 0)
    value_rows = bell_draw(key_of[2], (BLOCKS, BLOCK_LEN, KV_HEADS * HEAD_DIM), 1.0, 6.0, ((0, 16), (1, 16)))
    tile_segment = jnp.searchsorted(jnp.cumsum(ragged_sizes(key_of[3], TILES // 4, TILES, 8, 0)), jnp.arange(TILES), side="right").astype(jnp.int32)
    return dict(queries=queries, key_rows=key_rows, value_rows=value_rows, tile_segment=tile_segment)


masked_score = -1.0e30


def visible(query_pos, query_seg, key_pos, key_seg):
    earlier = key_pos[None, :] <= query_pos[:, None]
    same_image = (key_seg[None, :] == query_seg[:, None]) & (query_seg[:, None] % 2 == 1)
    return earlier | same_image


def reference(queries, key_rows, value_rows, tile_segment):
    seq_total = queries.shape[0] * queries.shape[1]
    group_size = Q_HEADS // KV_HEADS
    query_flat = queries.reshape(seq_total, KV_HEADS, group_size, HEAD_DIM)
    key_flat = key_rows.reshape(seq_total, KV_HEADS, HEAD_DIM).astype(jnp.float32)
    value_flat = value_rows.reshape(seq_total, KV_HEADS, HEAD_DIM).astype(jnp.float32)
    positions = jnp.arange(seq_total, dtype=jnp.int32)
    segments = tile_segment[positions // TILE]
    block_rows = math.gcd(seq_total, 128)
    score_scale = HEAD_DIM ** -0.5

    def one_block(block_index):
        begin = (block_index * block_rows).astype(jnp.int32)
        query_block = lax.dynamic_slice_in_dim(query_flat, begin, block_rows, 0).astype(jnp.float32)
        query_pos = begin + jnp.arange(block_rows, dtype=jnp.int32)
        query_seg = lax.dynamic_slice_in_dim(segments, begin, block_rows, 0)
        allowed = visible(query_pos, query_seg, positions, segments)
        scores = jnp.einsum("qkgd,skd->kgqs", query_block, key_flat) * score_scale
        scores = jnp.where(allowed[None, None], scores, masked_score)
        new_max = jnp.max(scores, axis=3)
        weights = jnp.where(allowed[None, None], jnp.exp(scores - new_max[..., None]), 0.0)
        denominators = jnp.sum(weights, axis=3)
        rounded = lax.optimization_barrier(weights.astype(jnp.bfloat16))
        mixed = jnp.einsum("kgqs,skd->kgqd", rounded.astype(jnp.float32), value_flat) / denominators[..., None]
        return jnp.transpose(mixed, (2, 0, 1, 3)).reshape(block_rows, Q_HEADS * HEAD_DIM).astype(jnp.bfloat16)

    blocks_out = lax.map(one_block, jnp.arange(seq_total // block_rows, dtype=jnp.int32))
    return blocks_out.reshape(queries.shape)
```

```python
import math

import jax
import jax.numpy as jnp
from jax import lax
from jax.experimental import pallas as pl
from jax.experimental.pallas import tpu as pltpu
from jax.sharding import Mesh, PartitionSpec as P

HEAD_DIM = 128
TILE = 128
HALF = 512
MASKED = -1e30
START = -1e29
OFFS = (0, -1, 1, 2)
X = ("xh", "xl")
BLK = ("y", "xl", "core")
RIGHT = [(i, (i + 1) % 4) for i in range(4)]
LEFT = [(i, (i - 1) % 4) for i in range(4)]


def ring(rows, axes):
    half = rows.shape[0] // 2
    right = lax.ppermute(rows, axes, RIGHT)
    left = lax.ppermute(rows, axes, LEFT)
    far_a = lax.ppermute(right[:half], axes, RIGHT)
    far_b = lax.ppermute(left[half:], axes, LEFT)
    return [rows, right, left, far_a, far_b]


def attend(seg_ref, idx_ref, qo_ref, qm_ref, *rest):
    kv_refs = rest[:20]
    oo_ref, om_ref, buf, qs, acc, mx, sems = rest[20:]
    b, xh, xl, y, core = [idx_ref[k] for k in range(5)]
    x = xh * 2 + xl

    k = 0
    for c in range(2):
        cc = core ^ c
        for half in range(2):
            piece = 0
            for part in range(5):
                ref = kv_refs[k]
                k += 1
                for p in range(ref.shape[0] // 256):
                    outer, inner = OFFS[piece // 4], OFFS[piece % 4]
                    piece += 1
                    dx, dy = (inner, outer) if half == 0 else (outer, inner)
                    sx = (x + dx) & 3
                    sy = (y + dy) & 3
                    sb = sy * 4 + (sx & 1) * 2 + cc
                    slot = (sb * 2 + half) * 2 + (sx >> 1)
                    pltpu.make_async_copy(
                        ref.at[pl.ds(p * 256, 256)], buf.at[slot], sems.at[slot]
                    ).start()

    scale = HEAD_DIM ** -0.5 * math.log2(math.e)
    for t in range(8):
        src = qo_ref if t < 4 else qm_ref
        rows = src[t % 4].astype(jnp.float32) * scale
        rows = jnp.concatenate([rows[:, h * 128:(h + 1) * 128] for h in range(4)], axis=0)
        hi = rows.astype(jnp.bfloat16)
        lo = (rows - hi.astype(jnp.float32)).astype(jnp.bfloat16)
        qs[t] = jnp.concatenate([hi, lo], axis=1)
    acc[...] = jnp.zeros_like(acc)
    mx[...] = jnp.full_like(mx, START)

    def tile_of(t):
        return b * 8 + t if t < 4 else (15 - b) * 8 + t

    limits = []
    for t in range(8):
        qt = tile_of(t)
        seg = seg_ref[qt]
        end = qt
        for d in range(1, 8):
            nxt = jnp.minimum(qt + d, 127)
            end = end + jnp.where((seg_ref[nxt] == seg) & (qt + d < 128), 1, 0)
        limits.append(jnp.where((seg & 1) == 1, (end + 1) * TILE - 1, -1))

    def step(t, kk, vv, mask):
        s = lax.dot_general(qs[t], kk, (((1,), (1,)), ((), ())), preferred_element_type=jnp.float32)
        if mask is not None:
            s = jnp.where(mask, s, MASKED)
        old = mx[t]
        new = jnp.maximum(old, jnp.max(s, axis=1, keepdims=True))
        alpha = jnp.exp2(old - new)
        p = jnp.exp2(s - jnp.concatenate([new] * (s.shape[1] // 128), axis=1)).astype(jnp.bfloat16)
        pv = jnp.dot(p, vv, preferred_element_type=jnp.float32)
        acc[t] = acc[t] * jnp.concatenate([alpha, alpha], axis=1) + pv
        mx[t] = new

    def load(slot, n):
        rows = buf[pl.ds(slot, n)].reshape(n * 256, 256)
        keys, vals = rows[:, :128], rows[:, 128:]
        kk = jnp.concatenate([keys, keys], axis=1)
        vv = jnp.concatenate([vals, jnp.ones_like(vals)], axis=1)
        return kk, vv

    def wait(slot, n):
        for i in range(n):
            pltpu.make_async_copy(kv_refs[0].at[pl.ds(0, 256)], buf.at[slot + i], sems.at[slot + i]).wait()

    def wait_all(i, c):
        wait(i * 4, 4)
        return c

    lax.fori_loop(0, 16, wait_all, 0)

    for g in range(2):
        base = b if g == 0 else 15 - b

        def dense(j, c):
            kk, vv = load(j * 4, 4)
            for t in range(4):
                step(g * 4 + t, kk, vv, None)
            return c

        lax.fori_loop(0, base, dense, 0)

        last = base * 2 + g
        for t in range(4):
            last = jnp.maximum(last, limits[g * 4 + t] // HALF)

        def masked(j, c):
            kk, vv = load(j * 2, 2)
            col = lax.broadcasted_iota(jnp.int32, (256, HALF), 1)
            row = lax.broadcasted_iota(jnp.int32, (256, HALF), 0)
            kpos = j * HALF + ((col & 255) >> 6) * TILE + (col >> 8) * 64 + (col & 63)
            for t in range(4):
                qpos = tile_of(g * 4 + t) * TILE + xh * 64 + (row & 63)
                step(g * 4 + t, kk, vv, kpos <= jnp.maximum(qpos, limits[g * 4 + t]))
            return c

        lax.fori_loop(base * 2, last + 1, masked, 0)

    for t in range(8):
        dst = oo_ref if t < 4 else om_ref
        a = acc[t]
        o = (a[:, :128] / a[:, 128:]).astype(jnp.bfloat16)
        dst[t % 4] = jnp.concatenate([o[h * 64:(h + 1) * 64] for h in range(4)], axis=1)


def local(queries, key_rows, value_rows, tile_segment):
    xh, xl, y, core = [lax.axis_index(a) for a in ("xh", "xl", "y", "core")]
    b = y * 4 + xl * 2 + core
    q = queries[0].reshape(64, 8, 512)
    k = key_rows[0].reshape(64, 8, 128)
    v = value_rows[0].reshape(64, 8, 128)
    qkv = jnp.transpose(jnp.concatenate([k, v, q], axis=2), (1, 0, 2))
    qkv = lax.all_to_all(qkv, "z", split_axis=0, concat_axis=0, tiled=True)
    kv = qkv[:, :, :256].reshape(512, 256)
    q = qkv[:, :, 256:]

    mirror = [(i, 15 - i) for i in range(16)]
    qo = q[:4]
    qm = lax.ppermute(q[4:], BLK, mirror)

    rows_a = jnp.concatenate(ring(kv[:256], X), axis=0)
    rows_b = jnp.concatenate(ring(kv[256:], "y"), axis=0)
    parts = ring(rows_a, "y") + ring(rows_b, X)
    swap = [lax.ppermute(p, "core", [(0, 1), (1, 0)]) for p in parts]

    idx = jnp.stack([b, xh, xl, y, core]).astype(jnp.int32)
    tile = jax.ShapeDtypeStruct((4, 64, 512), jnp.bfloat16)
    smem = pl.BlockSpec(memory_space=pltpu.SMEM)
    vmem = pl.BlockSpec(memory_space=pltpu.VMEM)
    oo, om = pl.pallas_call(
        attend,
        out_shape=(tile, tile),
        in_specs=[smem, smem, vmem, vmem] + [pl.BlockSpec(memory_space=pl.ANY)] * 20,
        out_specs=(vmem, vmem),
        scratch_shapes=[
            pltpu.VMEM((64, 256, 256), jnp.bfloat16),
            pltpu.VMEM((8, 256, 256), jnp.bfloat16),
            pltpu.VMEM((8, 256, 256), jnp.float32),
            pltpu.VMEM((8, 256, 128), jnp.float32),
            pltpu.SemaphoreType.DMA((64,)),
        ],
        name="attend",
    )(tile_segment, idx, qo, qm, *parts, *swap)

    om = lax.ppermute(om, BLK, mirror)
    out = jnp.concatenate([oo, om], axis=0)
    out = lax.all_to_all(out, "z", split_axis=0, concat_axis=0, tiled=True)
    return jnp.transpose(out, (1, 0, 2)).reshape(1, 64, 4096)


def solution(mesh):
    fine = Mesh(mesh.devices.reshape(8, 2, 4, 2, 2), ("z", "xh", "y", "xl", "core"))
    split = P(BLK, ("z", "xh"), None)
    return jax.shard_map(
        local, mesh=fine, in_specs=(split, split, split, P()), out_specs=split, check_vma=False
    )
```

```python
import math

import jax
import jax.numpy as jnp
from jax import lax
from jax.experimental import pallas as pl
from jax.experimental.pallas import tpu as pltpu
from jax.sharding import Mesh, PartitionSpec as P


HEAD_DIM = 128
TILE = 128
HALF = 512
COLS = 1024
MASKED = -1e30
SLACK = 60.0
OFFS = (0, -1, 1, 2)
PLANE = ("xh", "y", "xl", "core")
ROUND = ("z", "y", "xl", "core")
TEAMS = [[z * 16 + (n if z < 4 else 15 - n) for z in range(8)] for n in range(16)]


def exchange(rows):
    return lax.all_to_all(
        rows, ROUND, split_axis=0, concat_axis=0, axis_index_groups=TEAMS, tiled=True
    )


def plane_perm(step, x_core):
    pairs = []
    for xh in range(2):
        for y in range(4):
            for xl in range(2):
                for core in range(2):
                    x = xh * 2 + xl
                    tx, ty = ((x + step) % 4, y) if core == x_core else (x, (y + step) % 4)
                    src = ((xh * 4 + y) * 2 + xl) * 2 + core
                    dst = (((tx // 2) * 4 + ty) * 2 + tx % 2) * 2 + core
                    pairs.append((src, dst))
    return pairs


def ring_near(rows, x_core):
    return (
        lax.ppermute(rows, PLANE, plane_perm(1, x_core)),
        lax.ppermute(rows, PLANE, plane_perm(-1, x_core)),
    )


def ring_far(right, left, x_core):
    half = right.shape[0] // 2
    return (
        lax.ppermute(right[:half], PLANE, plane_perm(1, x_core)),
        lax.ppermute(left[half:], PLANE, plane_perm(-1, x_core)),
    )


def swap(rows):
    return lax.ppermute(rows, "core", [(0, 1), (1, 0)])


ALL8 = [(o, j) for o in range(4) for j in range(2)]
PARTS = (
    (0, 0, 0, ALL8, 0),
    (1, 0, 1, ALL8, 2), (2, 0, 2, ALL8, 4),
    (1, 1, 1, ALL8, 6), (2, 1, 2, ALL8, 6),
    (0, 1, 0, ALL8, 10), (3, 1, 3, ALL8[:4], 10), (4, 1, 3, ALL8[4:], 10),
    (3, 0, 3, ALL8[:4], 14), (4, 0, 3, ALL8[4:], 14),
)


def attend(seg_ref, idx_ref, q_ref, self_ref, *rest):
    own_refs, swp_refs = rest[:5], rest[5:10]
    o_ref, buf, qs, hbs, far, flag, sems, acc, mx, over, lim = rest[10:]
    z, xh, xl, y, core = [idx_ref[k] for k in range(5)]
    flip = jnp.where(z < 4, 0, 15)
    x = xh * 2 + xl
    n = (y * 4 + xl * 2 + core) ^ flip

    for op, half, o2, pieces, base in PARTS:
        for i, (o1, j) in enumerate(pieces):
            dx, dy = (OFFS[o1], OFFS[o2]) if half == 0 else (OFFS[o2], OFFS[o1])
            sx, sy = (x + dx) & 3, (y + dy) & 3
            cc = half ^ j
            pair = base + (sx & 1 if half == 0 else sy)
            block = (sy * 4 + (sx & 1) * 2 + cc) ^ flip ^ (15 * half)
            hbs[pair * 2 + cc] = block * 2 + half
            slot = pair * 4 + cc * 2 + (sx >> 1)

            @pl.when(core == half)
            def _():
                pltpu.make_async_copy(
                    own_refs[op].at[pl.ds(i * 256, 256)], buf.at[slot], sems.at[slot]
                ).start()

            @pl.when(core != half)
            def _():
                pltpu.make_async_copy(
                    swp_refs[op].at[pl.ds(i * 256, 256)], buf.at[slot], sems.at[slot]
                ).start()

    scale = HEAD_DIM ** -0.5 * math.log2(math.e)
    for g in range(2):
        reach = n * 2 if g == 0 else (15 - n) * 2 + 1
        for t in range(4):
            rows = q_ref[g * 4 + t].astype(jnp.float32) * scale
            cols = jnp.concatenate([rows[:, h * 128:(h + 1) * 128] for h in range(4)], axis=0).T
            keys = self_ref[g * 4 + t][:, :128].astype(jnp.float32)
            keys = jnp.concatenate([keys] * 4, axis=0).T
            hi = cols.astype(jnp.bfloat16)
            lo = (cols - hi.astype(jnp.float32)).astype(jnp.bfloat16)
            at = slice(t * 256, (t + 1) * 256)
            qs[g, :, at] = jnp.concatenate([hi, lo], axis=0)
            mx[g, :, at] = jnp.sum(cols * keys, axis=0, keepdims=True)
            qt = (n if g == 0 else 15 - n) * 8 + g * 4 + t
            seg = seg_ref[qt]
            end = qt
            for d in range(1, 8):
                nxt = jnp.minimum(qt + d, 127)
                end = end + jnp.where((seg_ref[nxt] == seg) & (qt + d < 128), 1, 0)
            limit = jnp.where((seg & 1) == 1, (end + 1) * TILE - 1, -1)
            reach = jnp.maximum(reach, limit // HALF)
            col = lax.broadcasted_iota(jnp.int32, (1, 256), 1)
            lim[g, :, at] = jnp.maximum(qt * TILE + xh * 64 + (col & 63), limit)
        far[g] = reach
    acc[...] = jnp.zeros_like(acc)

    def load(slot, count):
        rows = buf[pl.ds(slot, count)].reshape(count * 256, 256)
        keys = rows[:, :128]
        ones = jnp.ones((16, count * 256), jnp.bfloat16)
        return (
            jnp.concatenate([keys, keys], axis=1),
            jnp.concatenate([rows[:, 128:].T, ones], axis=0),
        )

    def scores(g, kk, mask):
        s = jnp.dot(kk, qs[g], preferred_element_type=jnp.float32)
        return s if mask is None else jnp.where(mask, s, MASKED)

    def by_sublane(a):
        return a.reshape(a.shape[0] // 8, 8, COLS)

    def quick(g, kk, vt, mask):
        ref = mx[g]
        s = scores(g, kk, mask)
        top = jnp.max(by_sublane(s), axis=0)
        p = jnp.exp2(s - ref)
        pv = jnp.dot(vt, p.astype(jnp.bfloat16), preferred_element_type=jnp.float32)
        top = jnp.max(top, axis=0, keepdims=True) - ref
        over[...] = top
        good = top <= SLACK
        acc[g] = acc[g] + jnp.where(good, pv, 0.0)
        flag[0] = (jnp.max(top) > SLACK).astype(jnp.int32)

    def slow(g, kk, vt, mask):
        todo = over[...] > SLACK
        s = scores(g, kk, mask)
        old = mx[g]
        new = jnp.where(todo, jnp.maximum(old, jnp.max(s, axis=0, keepdims=True)), old)
        alpha = jnp.exp2(old - new)
        p = jnp.where(todo, jnp.exp2(s - new), 0.0)
        pv = jnp.dot(vt, p.astype(jnp.bfloat16), preferred_element_type=jnp.float32)
        acc[g] = acc[g] * alpha + pv
        mx[g] = new

    def both(g, slot, count, mask):
        quick(g, *load(slot, count), mask)

        @pl.when(flag[0] == 1)
        def _():
            slow(g, *load(slot, count), mask)

    def one_pair(p, c):
        for i in range(4):
            pltpu.make_async_copy(
                own_refs[0].at[pl.ds(0, 256)], buf.at[p * 4 + i], sems.at[p * 4 + i]
            ).wait()
        hb0, hb1 = hbs[p * 2], hbs[p * 2 + 1]

        def one_group(g, c):
            hbq = jnp.where(g == 0, n * 2, (15 - n) * 2 + 1)
            dense = (hb0 < hbq) & (hb1 < hbq)

            @pl.when(dense)
            def _():
                both(g, p * 4, 4, None)

            @pl.when(jnp.logical_not(dense))
            def _():
                def masked(u, c):
                    hb = hbs[p * 2 + u]

                    @pl.when(hb <= far[g])
                    def _():
                        key = lax.broadcasted_iota(jnp.int32, (HALF, 128), 0)
                        kpos = hb * HALF + ((key & 255) >> 6) * TILE + (key >> 8) * 64 + (key & 63)
                        kpos = jnp.concatenate([kpos] * (COLS // 128), axis=1)
                        both(g, p * 4 + u * 2, 2, kpos <= lim[g])

                    return c

                lax.fori_loop(0, 2, masked, 0)

            return c

        lax.fori_loop(0, 2, one_group, 0)
        return c

    lax.fori_loop(0, 16, one_pair, 0)

    for t in range(8):
        at = slice(t % 4 * 256, (t % 4 + 1) * 256)
        total = acc[t // 4, 128:129, at]
        o = (acc[t // 4, :128, at] / total).T.astype(jnp.bfloat16)
        o_ref[t] = jnp.concatenate([o[h * 64:(h + 1) * 64] for h in range(4)], axis=1)


def local(queries, key_rows, value_rows, tile_segment):
    z, xh, xl, y, core = [lax.axis_index(a) for a in ("z", "xh", "xl", "y", "core")]
    q = queries[0].reshape(64, 8, 512)
    k = key_rows[0].reshape(64, 8, 128)
    v = value_rows[0].reshape(64, 8, 128)
    kept_kv = exchange(jnp.transpose(jnp.concatenate([k, v], axis=2), (1, 0, 2)))
    kv = kept_kv.reshape(512, 256)
    idx = jnp.stack([z, xh, xl, y, core]).astype(jnp.int32)

    kept = lax.dynamic_slice_in_dim(kv, core * 256, 256, 0)
    sent = lax.dynamic_slice_in_dim(kv, (1 - core) * 256, 256, 0)
    start = jnp.concatenate([kept, swap(sent)], axis=0)
    q = jnp.transpose(q, (1, 0, 2))
    q, start = lax.optimization_barrier((q, start))
    q = exchange(q)
    r1, l1 = ring_near(start, 0)
    f1 = ring_far(r1, l1, 0)
    row = jnp.concatenate([start, r1, l1, *f1], axis=0)
    r2, l2 = ring_near(row, 1)
    row_s = swap(row)
    f2 = ring_far(r2, l2, 1)
    own = (row, r2, l2, *f2)
    swp = (row_s, *[swap(o) for o in own[1:]])

    smem = pl.BlockSpec(memory_space=pltpu.SMEM)
    vmem = pl.BlockSpec(memory_space=pltpu.VMEM)
    out = pl.pallas_call(
        attend,
        out_shape=jax.ShapeDtypeStruct((8, 64, 512), jnp.bfloat16),
        in_specs=[smem, smem, vmem, vmem] + [pl.BlockSpec(memory_space=pl.ANY)] * 10,
        out_specs=vmem,
        scratch_shapes=[
            pltpu.VMEM((64, 256, 256), jnp.bfloat16),
            pltpu.VMEM((2, 256, COLS), jnp.bfloat16),
            pltpu.SMEM((32,), jnp.int32),
            pltpu.SMEM((2,), jnp.int32),
            pltpu.SMEM((1,), jnp.int32),
            pltpu.SemaphoreType.DMA((64,)),
            pltpu.VMEM((2, 144, COLS), jnp.float32),
            pltpu.VMEM((2, 1, COLS), jnp.float32),
            pltpu.VMEM((1, COLS), jnp.float32),
            pltpu.VMEM((2, 1, COLS), jnp.int32),
        ],
        name="attend",
    )(tile_segment, idx, q, kept_kv, *own, *swp)

    out = exchange(out)
    return jnp.transpose(out, (1, 0, 2)).reshape(1, 64, 4096)


def solution(mesh):
    fine = Mesh(mesh.devices.reshape(8, 2, 4, 2, 2), ("z", "xh", "y", "xl", "core"))
    split = P(("y", "xl", "core"), ("z", "xh"), None)

    return jax.shard_map(
        local, mesh=fine, in_specs=(split, split, split, P()), out_specs=split, check_vma=False
    )
```

```python
import math

import jax
import jax.numpy as jnp
from jax import lax
from jax.experimental import pallas as pl
from jax.experimental.pallas import tpu as pltpu
from jax.sharding import Mesh, PartitionSpec as P


HEAD_DIM = 128
TILE = 128
HALF = 512
COLS = 1024
MASKED = -1e30
START = -1e29
SLACK = 60.0
OFFS = (0, -1, 1, 2)
PLANE = ("xh", "y", "xl", "core")
ROUND = ("z", "y", "xl", "core")
TEAMS = [[z * 16 + (n if z < 4 else 15 - n) for z in range(8)] for n in range(16)]


def exchange(rows):
    return lax.all_to_all(
        rows, ROUND, split_axis=0, concat_axis=0, axis_index_groups=TEAMS, tiled=True
    )


def plane_perm(step, x_core):
    pairs = []
    for xh in range(2):
        for y in range(4):
            for xl in range(2):
                for core in range(2):
                    x = xh * 2 + xl
                    tx, ty = ((x + step) % 4, y) if core == x_core else (x, (y + step) % 4)
                    src = ((xh * 4 + y) * 2 + xl) * 2 + core
                    dst = (((tx // 2) * 4 + ty) * 2 + tx % 2) * 2 + core
                    pairs.append((src, dst))
    return pairs


def ring_near(rows, x_core):
    return (
        lax.ppermute(rows, PLANE, plane_perm(1, x_core)),
        lax.ppermute(rows, PLANE, plane_perm(-1, x_core)),
    )


def ring_far(right, left, x_core):
    half = right.shape[0] // 2
    return (
        lax.ppermute(right[:half], PLANE, plane_perm(1, x_core)),
        lax.ppermute(left[half:], PLANE, plane_perm(-1, x_core)),
    )


def swap(rows):
    return lax.ppermute(rows, "core", [(0, 1), (1, 0)])


ALL8 = [(o, j) for o in range(4) for j in range(2)]
A4, B4 = ALL8[:4], ALL8[4:]
PARTS = (
    (0, 0, 0, A4, 0), (1, 0, 0, B4, 0),
    (2, 0, 1, A4, 2), (4, 0, 1, B4, 2), (3, 0, 2, A4, 4), (5, 0, 2, B4, 4),
    (2, 1, 1, A4, 6), (4, 1, 1, B4, 6), (3, 1, 2, A4, 6), (5, 1, 2, B4, 6),
    (0, 1, 0, A4, 10), (1, 1, 0, B4, 10), (6, 1, 3, A4, 10), (7, 1, 3, B4, 10),
    (6, 0, 3, A4, 14), (7, 0, 3, B4, 14),
)


def attend(seg_ref, idx_ref, q_ref, self_ref, *rest):
    own_refs, swp_refs = rest[:8], rest[8:16]
    o_ref, buf, qs, hbs, far, flag, sems, acc, mx, over, lim = rest[16:]
    z, xh, xl, y, core = [idx_ref[k] for k in range(5)]
    flip = jnp.where(z < 4, 0, 15)
    x = xh * 2 + xl
    n = (y * 4 + xl * 2 + core) ^ flip

    for op, half, o2, pieces, base in PARTS:
        for i, (o1, j) in enumerate(pieces):
            dx, dy = (OFFS[o1], OFFS[o2]) if half == 0 else (OFFS[o2], OFFS[o1])
            sx, sy = (x + dx) & 3, (y + dy) & 3
            cc = half ^ j
            pair = base + (sx & 1 if half == 0 else sy)
            block = (sy * 4 + (sx & 1) * 2 + cc) ^ flip ^ (15 * half)
            hbs[pair * 2 + cc] = block * 2 + half
            slot = pair * 4 + cc * 2 + (sx >> 1)

            @pl.when(core == half)
            def _():
                pltpu.make_async_copy(
                    own_refs[op].at[pl.ds(i * 256, 256)], buf.at[slot], sems.at[slot]
                ).start()

            @pl.when(core != half)
            def _():
                pltpu.make_async_copy(
                    swp_refs[op].at[pl.ds(i * 256, 256)], buf.at[slot], sems.at[slot]
                ).start()

    scale = HEAD_DIM ** -0.5 * math.log2(math.e)
    for g in range(2):
        reach = n * 2 if g == 0 else (15 - n) * 2 + 1
        for t in range(4):
            rows = q_ref[g * 4 + t].astype(jnp.float32) * scale
            cols = jnp.concatenate([rows[:, h * 128:(h + 1) * 128] for h in range(4)], axis=0).T
            keys = self_ref[g * 4 + t][:, :128].astype(jnp.float32)
            keys = jnp.concatenate([keys] * 4, axis=0).T
            hi = cols.astype(jnp.bfloat16)
            lo = (cols - hi.astype(jnp.float32)).astype(jnp.bfloat16)
            at = slice(t * 256, (t + 1) * 256)
            qs[g, :, at] = jnp.concatenate([hi, lo], axis=0)
            mx[g, :, at] = jnp.sum(cols * keys, axis=0, keepdims=True)
            qt = (n if g == 0 else 15 - n) * 8 + g * 4 + t
            seg = seg_ref[qt]
            end = qt
            for d in range(1, 8):
                nxt = jnp.minimum(qt + d, 127)
                end = end + jnp.where((seg_ref[nxt] == seg) & (qt + d < 128), 1, 0)
            limit = jnp.where((seg & 1) == 1, (end + 1) * TILE - 1, -1)
            reach = jnp.maximum(reach, limit // HALF)
            col = lax.broadcasted_iota(jnp.int32, (1, 256), 1)
            lim[g, :, at] = jnp.maximum(qt * TILE + xh * 64 + (col & 63), limit)
        far[g] = reach
    acc[...] = jnp.zeros_like(acc)
    over[...] = jnp.full_like(over, MASKED)

    def load(slot, count):
        rows = buf[pl.ds(slot, count)].reshape(count * 256, 256)
        keys = rows[:, :128]
        ones = jnp.ones((16, count * 256), jnp.bfloat16)
        return (
            jnp.concatenate([keys, keys], axis=1),
            jnp.concatenate([rows[:, 128:].T, ones], axis=0),
        )

    def scores(g, kk, mask):
        s = jnp.dot(kk, qs[g], preferred_element_type=jnp.float32)
        return s if mask is None else jnp.where(mask, s, MASKED)

    def by_sublane(a):
        return a.reshape(a.shape[0] // 8, 8, COLS)

    def quick(g, kk, vt, mask):
        s = scores(g, kk, mask)
        over[g] = jnp.maximum(over[g], jnp.max(by_sublane(s), axis=0))
        p = jnp.exp2(s - mx[g])
        acc[g] = acc[g] + jnp.dot(vt, p.astype(jnp.bfloat16), preferred_element_type=jnp.float32)

    def slow(g, kk, vt, mask):
        s = scores(g, kk, mask)
        old = mx[g]
        new = jnp.maximum(old, jnp.max(s, axis=0, keepdims=True))
        p = jnp.exp2(s - new)
        pv = jnp.dot(vt, p.astype(jnp.bfloat16), preferred_element_type=jnp.float32)
        acc[g] = acc[g] * jnp.exp2(old - new) + pv
        mx[g] = new

    def masked(g, unit, apply):
        hb = hbs[unit]

        @pl.when(hb <= far[g])
        def _():
            key = lax.broadcasted_iota(jnp.int32, (HALF, 128), 0)
            kpos = hb * HALF + ((key & 255) >> 6) * TILE + (key >> 8) * 64 + (key & 63)
            kpos = jnp.concatenate([kpos] * (COLS // 128), axis=1)
            apply(g, *load(unit * 2, 2), kpos <= lim[g])

    def one_pair(p, c):
        for i in range(4):
            pltpu.make_async_copy(
                own_refs[0].at[pl.ds(0, 256)], buf.at[p * 4 + i], sems.at[p * 4 + i]
            ).wait()
        hb = jnp.maximum(hbs[p * 2], hbs[p * 2 + 1])
        first, second = hb < n * 2, hb < (15 - n) * 2 + 1

        @pl.when(first & second)
        def _():
            kk, vt = load(p * 4, 4)
            quick(0, kk, vt, None)
            quick(1, kk, vt, None)

        @pl.when(jnp.logical_not(first & second))
        def _():
            def one_group(g, c):
                dense = jnp.where(g == 0, first, second)

                @pl.when(dense)
                def _():
                    quick(g, *load(p * 4, 4), None)

                @pl.when(jnp.logical_not(dense))
                def _():
                    def one_unit(u, c):
                        masked(g, p * 2 + u, quick)
                        return c

                    lax.fori_loop(0, 2, one_unit, 0)

                return c

            lax.fori_loop(0, 2, one_group, 0)

        return c

    lax.fori_loop(0, 16, one_pair, 0)

    excess = jnp.maximum(
        jnp.max(over[0], axis=0, keepdims=True) - mx[0],
        jnp.max(over[1], axis=0, keepdims=True) - mx[1],
    )
    flag[0] = (jnp.max(excess) > SLACK).astype(jnp.int32)

    @pl.when(flag[0] == 1)
    def _():
        acc[...] = jnp.zeros_like(acc)
        mx[...] = jnp.full_like(mx, START)

        def again(i, c):
            masked(i & 1, i >> 1, slow)
            return c

        lax.fori_loop(0, 64, again, 0)

    for t in range(8):
        at = slice(t % 4 * 256, (t % 4 + 1) * 256)
        total = acc[t // 4, 128:129, at]
        o = (acc[t // 4, :128, at] / total).T.astype(jnp.bfloat16)
        o_ref[t] = jnp.concatenate([o[h * 64:(h + 1) * 64] for h in range(4)], axis=1)


def local(queries, key_rows, value_rows, tile_segment):
    z, xh, xl, y, core = [lax.axis_index(a) for a in ("z", "xh", "xl", "y", "core")]
    q = queries[0].reshape(64, 8, 512)
    k = key_rows[0].reshape(64, 8, 128)
    v = value_rows[0].reshape(64, 8, 128)
    kept_kv = exchange(jnp.transpose(jnp.concatenate([k, v], axis=2), (1, 0, 2)))
    kv = kept_kv.reshape(512, 256)
    idx = jnp.stack([z, xh, xl, y, core]).astype(jnp.int32)

    kept = lax.dynamic_slice_in_dim(kv, core * 256, 256, 0)
    sent = lax.dynamic_slice_in_dim(kv, (1 - core) * 256, 256, 0)
    start = jnp.concatenate([kept, swap(sent)], axis=0)
    q = jnp.transpose(q, (1, 0, 2))
    q, start = lax.optimization_barrier((q, start))
    q = exchange(q)
    r1, l1 = ring_near(start, 0)
    f1 = ring_far(r1, l1, 0)
    row_a = jnp.concatenate([start, r1], axis=0)
    row_b = jnp.concatenate([l1, *f1], axis=0)
    ra, la = ring_near(row_a, 1)
    rb, lb = ring_near(row_b, 1)
    fa = lax.ppermute(ra, PLANE, plane_perm(1, 1))
    fb = lax.ppermute(lb, PLANE, plane_perm(-1, 1))
    own = (row_a, row_b, ra, la, rb, lb, fa, fb)
    swp = tuple(swap(o) for o in own)

    smem = pl.BlockSpec(memory_space=pltpu.SMEM)
    vmem = pl.BlockSpec(memory_space=pltpu.VMEM)
    out = pl.pallas_call(
        attend,
        out_shape=jax.ShapeDtypeStruct((8, 64, 512), jnp.bfloat16),
        in_specs=[smem, smem, vmem, vmem] + [pl.BlockSpec(memory_space=pltpu.HBM)] * 16,
        out_specs=vmem,
        scratch_shapes=[
            pltpu.VMEM((64, 256, 256), jnp.bfloat16),
            pltpu.VMEM((2, 256, COLS), jnp.bfloat16),
            pltpu.SMEM((32,), jnp.int32),
            pltpu.SMEM((2,), jnp.int32),
            pltpu.SMEM((1,), jnp.int32),
            pltpu.SemaphoreType.DMA((64,)),
            pltpu.VMEM((2, 144, COLS), jnp.float32),
            pltpu.VMEM((2, 1, COLS), jnp.float32),
            pltpu.VMEM((2, 8, COLS), jnp.float32),
            pltpu.VMEM((2, 1, COLS), jnp.int32),
        ],
        name="attend",
    )(tile_segment, idx, q, kept_kv, *own, *swp)

    out = exchange(out)
    return jnp.transpose(out, (1, 0, 2)).reshape(1, 64, 4096)


def solution(mesh):
    fine = Mesh(mesh.devices.reshape(8, 2, 4, 2, 2), ("z", "xh", "y", "xl", "core"))
    split = P(("y", "xl", "core"), ("z", "xh"), None)

    return jax.shard_map(
        local, mesh=fine, in_specs=(split, split, split, P()), out_specs=split, check_vma=False
    )
```
